512 devices in a mesh: groups: 2 (over y), seq: 32 (over z, core), rep: 8 (over x).
Axes of the slice: x: 8, y: 2, z: 16, core: 2. Of those that a mesh axis runs over, the one named last changes fastest.
The devices are a block of a 8x16x16 slice.
Arguments:
- queries: bfloat16 [1024, 4096], P(('groups', 'seq'), 'rep'), parts along dimension 0, may hold values from -128 to 128
- keys_new: bfloat16 [1024, 1024], P(('groups', 'seq'), 'rep'), parts along dimension 0, may hold values from -4 to 4
- values_new: bfloat16 [1024, 1024], P(('groups', 'seq'), 'rep'), parts along dimension 0, may hold values from -6 to 6
- keys_past: bfloat16 [16384, 1024], P(('groups', 'seq'), 'rep'), parts along dimension 0, may hold values from -4 to 4
- values_past: bfloat16 [16384, 1024], P(('groups', 'seq'), 'rep'), parts along dimension 0, may hold values from -6 to 6
- block_order: int32 [64], P('groups'), parts along dimension 0, may hold values from 0 to 31, each once
- residual: bfloat16 [1024, 4096], P(('groups', 'seq'), 'rep'), parts along dimension 0, may hold values from -6 to 6
- out_proj: bfloat16 [4096, 4096], P('seq', 'rep'), may hold values from -0.09375 to 0.09375
- norm_gain: float32 [4096], replicated, may hold values from 0.5 to 1.5
- router: float32 [4096, 4], replicated, may hold values from -0.09375 to 0.09375
- w_gate: bfloat16 [8, 4096, 4096], P('rep', None, 'seq'), may hold values from -0.09375 to 0.09375
- w_up: bfloat16 [8, 4096, 4096], P('rep', None, 'seq'), may hold values from -0.09375 to 0.09375
- w_down: bfloat16 [8, 4096, 4096], P('rep', 'seq'), may hold values from -0.0625 to 0.0625
- expert_ids: int32 [1024, 2], P(('groups', 'seq')), parts along dimension 0, may hold values from 0 to 3, all different within a row; in each aligned block of 16 rows (0 to 15, 16 to 31, ...) at most 12 rows name the same one
Outputs:
- attended: bfloat16 [1024, 4096], P(('groups', 'seq'), 'rep'), parts along dimension 0
- layer_out: bfloat16 [1024, 4096], P(('groups', 'seq'), 'rep'), parts along dimension 0
- keys_cache: bfloat16 [1024, 1024], P(('groups', 'seq')), parts along dimension 0
- values_cache: bfloat16 [1024, 1024], P(('groups', 'seq')), parts along dimension 0
The draws below stay inside these ranges and needn't reach their ends.
There are 2 independent parts, one for each index of `groups`. The reference program is written for one: setup_inputs(seed, part) draws one part's arguments, and reference() takes and returns one part's arrays. A program takes and returns all parts, laid end to end along the dimension named above; an argument that names none is the same for every part. Nothing has to cross between parts.
Inputs may be any that keep to these rules, and one draw needn't show every extreme that they name: `block_order`: each block index 0 to 32 - 1 appears once. `expert_ids`: each row names 2 different experts; in the rows of one device (aligned blocks of 16 rows) no expert is named by more than 12 rows, and in some block one expert is named by exactly 12.
All inputs are finite; a program needn't handle non-finite values.
Results may differ from the reference program's by a relative error of at most 0.011.
Values may be sent and summed in bfloat16 or wider, within the bound.
A program may use at most 64 MiB of HBM per device.

```python
import math
import jax
import jax.numpy as jnp
import numpy as np
from jax import lax

D = 4096
HD = 128
Q_PER = 4
KV_HEADS = 8
HEADS = 32
EXPERTS = 4
TOP = 2
FF = 8192
TOK_DEV = 16
CAP = 12
HALVES = 2
S_NEW = 512
CTX = 8192
N_SEQ = 32


def drawn_pair(key):
    base = jax.random.fold_in(key, 11)
    key_seed, query_seed = jax.random.split(base)
    past_keys = jnp.clip(jax.random.normal(key_seed, (CTX, KV_HEADS * HD), jnp.float32), -4.0, 4.0)
    query_rows = jnp.clip(jax.random.normal(query_seed, (S_NEW, KV_HEADS * Q_PER * HD), jnp.float32), -4.0, 4.0)
    return (past_keys, query_rows)


def draw_queries(key, part):
    past_keys, query_rows = drawn_pair(key)
    return query_rows.astype(jnp.bfloat16)


def draw_keys_past(key, part):
    past_keys, query_rows = drawn_pair(key)
    return past_keys.astype(jnp.bfloat16)


def block_levels(own_key, shape, cuts, least, high):
    def one(dim, shards_of):
        draws = jax.random.uniform(jax.random.fold_in(jax.random.fold_in(own_key, 6), dim), (shards_of,), jnp.float32, least / len(cuts), high / len(cuts))
        return jnp.repeat(jnp.exp(draws), shape[dim] // shards_of).reshape((-1,) + (1,) * (len(shape) - dim - 1))

    loudness = one(*cuts[0])
    for cut in cuts[1:]:
        loudness = loudness * one(*cut)
    return loudness


def routed_block(key, own, number, rows, count, top, bound, lean):
    sequence = jax.random.permutation(key, count)
    heavy_load, usual = portions_of(count, rows * top, bound, lean, True), portions_of(count, rows * top, bound, lean, False)
    places = jnp.arange(count)

    def named(tallies, turn):
        used = int((tallies > 0).sum())
        fixed = max(1, used // 4)
        passed = fixed + (places - fixed + turn * (used - fixed)) % max(1, count - fixed)
        return jnp.zeros((count,), jnp.int32).at[sequence[jnp.where(places < fixed, places, passed)]].set(jnp.asarray(tallies, jnp.int32))

    tallies = jnp.where(number % 4 == 0, named(heavy_load, number // 4), named(usual, number - number // 4 - 1))
    mixed = jax.random.permutation(jax.random.fold_in(own, 3), count)
    giver, taker = mixed[0:count // 2 * 2:2], mixed[1:count // 2 * 2:2]
    room = jnp.minimum(tallies[giver] - 1, bound - tallies[taker]) // 2
    room = jnp.where((giver == sequence[0]) | (taker == sequence[0]) | (tallies[taker] == 0), 0, jnp.maximum(room, 0))
    passed = jax.random.randint(jax.random.fold_in(own, 4), (count // 2,), 0, 1 << 20) % (room + 1)
    tallies = tallies.at[giver].add(-passed).at[taker].add(passed)
    labels = jnp.searchsorted(jnp.cumsum(tallies), jnp.arange(rows * top), side="right").astype(jnp.int32)
    table = labels.reshape(top, rows).T
    table = table[jax.random.permutation(jax.random.fold_in(own, 1), rows)]
    turn = jax.random.randint(jax.random.fold_in(own, 2), (rows, 1), 0, top)
    return jnp.take_along_axis(table, (jnp.arange(top)[None, :] + turn) % top, axis=1)


def portions_of(amount, total, most, skew, full):
    loads = [(1 << 20) // math.isqrt(grade ** skew) + 1 for grade in range(1, amount + 1)]
    largest = most if full else min(most, max(-(-total // amount), total * loads[0] // sum(loads)))
    least = 1 if total - largest >= amount - 1 else 0
    given, spare = [largest] + [least] * (amount - 1), total - largest - least * (amount - 1)
    while spare > 0:
        movable = [i for i in range(1, amount) if given[i] < largest] or [i for i in range(1, amount) if given[i] < most]
        mass, remaining = sum([loads[i] for i in movable]), spare
        for i in movable:
            addition = min(most - given[i], max(1, remaining * loads[i] // mass), spare)
            given[i] = given[i] + addition
            spare = spare - addition
    return np.array(given)


def noise(stream_key, shape, scale, reach, cuts=(), kind=jnp.bfloat16):
    level = block_levels(stream_key, shape, cuts, -0.22, 0.18) if cuts else 1.0
    values = jax.random.normal(stream_key, shape, jnp.float32) * scale * level
    return jnp.minimum(jnp.maximum(values, -reach), reach).astype(kind)


def setup_inputs(seed: int = 0, part: int = 0) -> dict:
    streams_of = jax.random.split(jax.random.key(seed), 15)
    part_keys = jax.random.split(jax.random.fold_in(streams_of[14], part), 15)
    queries = draw_queries(jax.random.fold_in(jax.random.fold_in(streams_of[14], part), 71), part)
    keys_new = noise(part_keys[1], (S_NEW, KV_HEADS * HD), 1.0, 4.0, ((0, 32), (1, 8)))
    values_new = noise(part_keys[2], (S_NEW, KV_HEADS * HD), 1.0, 6.0, ((0, 32), (1, 8)))
    keys_past = draw_keys_past(jax.random.fold_in(jax.random.fold_in(streams_of[14], part), 71), part)
    values_past = noise(part_keys[4], (CTX, KV_HEADS * HD), 1.0, 6.0, ((0, 32), (1, 8)))
    block_order = jax.random.permutation(part_keys[5], N_SEQ).astype(jnp.int32)
    residual = noise(part_keys[6], (S_NEW, D), 1.0, 6.0, ((0, 32), (1, 8)))
    out_proj = noise(streams_of[7], (HEADS * HD, D), (HEADS * HD) ** -0.5, 0.09375, ((0, 32), (1, 8)))
    norm_gain = jnp.clip(1.0 + 0.1 * jax.random.normal(streams_of[8], (D,), jnp.float32), 0.5, 1.5)
    router = noise(streams_of[9], (D, EXPERTS), D ** -0.5, 0.09375, (), jnp.float32)
    w_gate = noise(streams_of[10], (EXPERTS * HALVES, D, FF // HALVES), D ** -0.5, 0.09375, ((0, 8), (2, 32)))
    w_up = noise(streams_of[11], (EXPERTS * HALVES, D, FF // HALVES), D ** -0.5, 0.09375, ((0, 8), (2, 32)))
    w_down = noise(streams_of[12], (EXPERTS * HALVES, FF // HALVES, D), FF ** -0.5, 0.0625, ((0, 8), (1, 32)))
    expert_ids_keys = jax.random.split(jax.random.fold_in(part_keys[13], 1), S_NEW // TOK_DEV)
    expert_ids_turns = jax.random.permutation(jax.random.fold_in(part_keys[13], 3), S_NEW // TOK_DEV)
    expert_ids = jax.vmap(lambda own, number: routed_block(jax.random.fold_in(part_keys[13], 2), own, number, TOK_DEV, EXPERTS, TOP, CAP, 2))(expert_ids_keys, expert_ids_turns).reshape((S_NEW, TOP))
    return {"queries": queries, "keys_new": keys_new, "values_new": values_new, "keys_past": keys_past, "values_past": values_past, "block_order": block_order, "residual": residual, "out_proj": out_proj, "norm_gain": norm_gain, "router": router, "w_gate": w_gate, "w_up": w_up, "w_down": w_down, "expert_ids": expert_ids}


def reference(queries, keys_new, values_new, keys_past, values_past, block_order, residual, out_proj, norm_gain, router, w_gate, w_up, w_down, expert_ids):
    token_index = jnp.arange(S_NEW, dtype=jnp.int32)
    position = block_order[token_index // TOK_DEV] * TOK_DEV + token_index % TOK_DEV
    new_visible = position[None, :] <= position[:, None]
    row_visible = jnp.concatenate([jnp.ones((S_NEW, CTX), dtype=bool), new_visible], axis=1)
    row_visible = jnp.repeat(row_visible, Q_PER, axis=0)
    query_heads = queries.reshape(S_NEW, KV_HEADS, Q_PER, HD).transpose(1, 0, 2, 3).reshape(KV_HEADS, S_NEW * Q_PER, HD)
    keys_all = jnp.concatenate([keys_past, keys_new], axis=0).reshape(CTX + S_NEW, KV_HEADS, HD).transpose(1, 0, 2)
    values_all = jnp.concatenate([values_past, values_new], axis=0).reshape(CTX + S_NEW, KV_HEADS, HD).transpose(1, 0, 2)

    def one_head(operands):
        query_block, key_block, value_block = operands
        scores = jnp.dot(query_block, key_block.T, preferred_element_type=jnp.float32) * (1.0 / math.sqrt(HD))
        highest = lax.optimization_barrier(jnp.max(jnp.where(row_visible, scores, -jnp.inf), axis=1, keepdims=True))
        weights = jnp.where(row_visible, jnp.exp(scores - highest), 0.0)
        numerator = jnp.dot(weights.astype(jnp.bfloat16), value_block, preferred_element_type=jnp.float32)
        return (numerator / lax.optimization_barrier(jnp.sum(weights, axis=1, keepdims=True))).astype(jnp.bfloat16)
    heads_out = lax.map(one_head, (query_heads, keys_all, values_all))
    attended_heads = heads_out.reshape(KV_HEADS, S_NEW, Q_PER * HD).transpose(1, 0, 2).reshape(S_NEW, KV_HEADS * Q_PER * HD)
    projected = jnp.dot(attended_heads, out_proj, preferred_element_type=jnp.float32)
    attended = (residual.astype(jnp.float32) + projected).astype(jnp.bfloat16)
    features = attended.astype(jnp.float32)
    mean_square = lax.optimization_barrier(jnp.mean(features * features, axis=1, keepdims=True))
    normed = (features * norm_gain[None, :] * lax.rsqrt(mean_square + 1e-05)).astype(jnp.bfloat16)
    logits = jnp.dot(normed.astype(jnp.float32), router, precision=lax.Precision.HIGHEST)
    expert_range = jnp.arange(EXPERTS, dtype=jnp.int32)
    first_pick = (expert_ids[:, 0:1] == expert_range[None, :]).astype(jnp.float32)
    second_pick = (expert_ids[:, 1:2] == expert_range[None, :]).astype(jnp.float32)
    share_first = jax.nn.sigmoid(lax.optimization_barrier(jnp.sum(first_pick * logits, axis=1)) - lax.optimization_barrier(jnp.sum(second_pick * logits, axis=1)))
    token_share = share_first[:, None] * first_pick + (1.0 - share_first)[:, None] * second_pick
    block_count = HALVES * N_SEQ
    block_width = FF // block_count
    mixture = jnp.zeros((S_NEW, D), jnp.float32)

    def add_block(running_sum, operands):
        act_piece, down_piece = operands
        partial_sum = jnp.dot(act_piece, down_piece, preferred_element_type=jnp.float32)
        rounded = lax.optimization_barrier(partial_sum.astype(jnp.bfloat16))
        return (running_sum + rounded.astype(jnp.float32), None)
    for expert in range(EXPERTS):
        gate_full = jnp.concatenate([w_gate[half_index * EXPERTS + expert] for half_index in range(HALVES)], axis=1)
        up_full = jnp.concatenate([w_up[half_index * EXPERTS + expert] for half_index in range(HALVES)], axis=1)
        down_full = jnp.concatenate([w_down[half_index * EXPERTS + expert] for half_index in range(HALVES)], axis=0)
        gate_part = jnp.dot(normed, gate_full, preferred_element_type=jnp.float32)
        up_part = jnp.dot(normed, up_full, preferred_element_type=jnp.float32)
        activation = (jax.nn.silu(gate_part) * up_part).astype(jnp.bfloat16)
        act_blocks = activation.reshape(S_NEW, block_count, block_width).transpose(1, 0, 2)
        down_blocks = down_full.reshape(block_count, block_width, D)
        expert_out, ignored = lax.scan(add_block, jnp.zeros((S_NEW, D), jnp.float32), (act_blocks, down_blocks))
        mixture = mixture + token_share[:, expert:expert + 1] * expert_out
    layer_out = (features + mixture).astype(jnp.bfloat16)
    return (attended, layer_out, keys_new, values_new)
```

```python
import functools
import math

import jax
import jax.numpy as jnp
from jax import lax
from jax.experimental import pallas as pl
from jax.experimental.pallas import tpu as pltpu
from jax.sharding import PartitionSpec as P

MESH = pl.DeviceIdType.MESH
BF16 = jnp.bfloat16
F32 = jnp.float32
EXPERTS = 4
CAP = 12
CORES = 2
STRIDES = 4


def iota(shape, dim):
    return lax.broadcasted_iota(jnp.int32, shape, dim)


def remote(src, dst, send, recv, device):
    return pltpu.make_async_remote_copy(
        src_ref=src,
        dst_ref=dst,
        send_sem=send,
        recv_sem=recv,
        device_id=device,
        device_id_type=MESH,
    )


def place():
    seq = lax.axis_index("seq")
    return seq // CORES, seq % CORES, lax.axis_index("rep")


def greet(devices):
    barrier = pltpu.get_barrier_semaphore()
    for device in devices:
        pl.semaphore_signal(barrier, inc=1, device_id=device, device_id_type=MESH)
    pl.semaphore_wait(barrier, len(devices))


def attention_kernel(
    nz,
    nr,
    order_ref,
    q_ref,
    kn_ref,
    vn_ref,
    kp_ref,
    vp_ref,
    res_ref,
    wo_ref,
    att_ref,
    full_ref,
    kc_ref,
    vc_ref,
    qbuf,
    qrows,
    kv,
    wall,
    osend,
    lsend,
    orecv,
    lrecv,
    oall,
    aall,
    kcs,
    vcs,
    loc,
    qs,
    qr,
    ks,
    kr,
    ds,
    dr,
    ws,
    wr,
    es,
    er,
    cs,
    cr,
    vs,
    vr,
    os_,
    or_,
    ls,
    lr,
    xs,
    xr,
    as_,
    ar,
):
    z, c, r = place()
    tok, width = q_ref.shape
    hd = kn_ref.shape[1]
    q_per = width // hd
    past = kp_ref.shape[0]
    half = past // 2
    block = past + tok
    first = tok + half
    stride = nz // STRIDES
    reach = stride // 2
    rows = tok * q_per
    window = kv.shape[1]
    depth = wo_ref.shape[0]
    scale = 1.0 / math.sqrt(hd)

    def at_z(offset, core=None):
        return lax.rem(z + (offset % nz), nz) * CORES + (c if core is None else core)

    def seq(offset, core=None):
        return {"seq": at_z(offset, core)}

    other = {"seq": z * CORES + (1 - c)}
    columns = [lax.rem(r + j, nr) for j in range(nr)]
    across = [{"rep": columns[j]} for j in range(nr)]

    def base(offset):
        return half + (offset + reach - 1) * block

    def kv_at(core, start, size):
        return kv.at[core, pl.ds(start, size), :]

    own = base(0)
    local = [
        pltpu.make_async_copy(q_ref, qbuf.at[0], loc.at[0]),
        pltpu.make_async_copy(kn_ref, kv.at[0, pl.ds(own, tok), pl.ds(0, hd)], loc.at[1]),
        pltpu.make_async_copy(vn_ref, kv.at[0, pl.ds(own, tok), pl.ds(hd, hd)], loc.at[2]),
        pltpu.make_async_copy(kp_ref, kv.at[0, pl.ds(own + tok, past), pl.ds(0, hd)], loc.at[3]),
        pltpu.make_async_copy(vp_ref, kv.at[0, pl.ds(own + tok, past), pl.ds(hd, hd)], loc.at[4]),
    ]

    def w_rows(offset, part=None):
        start = at_z(offset) * depth
        size = depth
        if part is not None:
            size = depth // 2
            start = start + part * size
        return wall.at[pl.ds(pl.multiple_of(start, depth // 2), size), :]

    w_local = pltpu.make_async_copy(wo_ref, w_rows(0), loc.at[5])
    for copy in local:
        copy.start()
    w_local.start()

    greet(
        [seq(1), seq(-1), other]
        + [seq(stride * j) for j in range(1, STRIDES)]
        + [across[j] for j in range(1, nr)]
    )
    pending = []

    def go(copy):
        copy.start()
        pending.append(copy)
        return copy

    local[0].wait()
    q_copies = {}
    for j in (2, 1, 3):
        slot = (STRIDES - j) % STRIDES
        q_copies[slot] = go(
            remote(qbuf.at[0], qbuf.at[slot], qs.at[slot], qr.at[slot], seq(stride * j))
        )
    for copy in local[1:]:
        copy.wait()
    k_right = {1: go(remote(kv_at(0, own, block), kv_at(0, base(-1), block), ks.at[0], kr.at[0], seq(1)))}
    k_left = {1: go(remote(kv_at(0, own, block), kv_at(0, base(1), block), ks.at[1], kr.at[1], seq(-1)))}

    dies = []

    def to_other(start, size):
        n = len(dies)
        dies.append(go(remote(kv_at(0, start, size), kv_at(1, start, size), ds.at[n], dr.at[n], other)))

    to_other(own, block)

    w_local.wait()

    def w_send(t):
        if t < nz // 2:
            return [
                (go(remote(w_rows(1 - t), w_rows(1 - t), ws.at[t], wr.at[t], seq(1))), -t, None),
                (go(remote(w_rows(t - 1), w_rows(t - 1), ws.at[nz - t], wr.at[nz - t], seq(-1))), t, None),
            ]
        return [
            (go(remote(w_rows(1 - t, 0), w_rows(1 - t, 0), ws.at[t], wr.at[t], seq(1))), -t, 0),
            (go(remote(w_rows(t - 1, 1), w_rows(t - 1, 1), ws.at[0], wr.at[0], seq(-1))), t, 1),
        ]

    w_dies = []

    def w_other(offset, part=None):
        n = len(w_dies)
        view = w_rows(offset, part)
        w_dies.append(go(remote(view, view, es.at[n], er.at[n], other)))

    flight = w_send(1)
    w_other(0)
    k_copies = []
    v_copies = []
    mine = pl.ds(pl.multiple_of(r * hd, hd), hd)
    for j in range(1, nr):
        k_copies.append(
            go(remote(kv.at[0, pl.ds(own, tok), pl.ds(0, hd)], kcs.at[:, mine], cs.at[j], cr.at[j], across[j]))
        )
        v_copies.append(
            go(remote(kv.at[0, pl.ds(own, tok), pl.ds(hd, hd)], vcs.at[:, mine], vs.at[j], vr.at[j], across[j]))
        )
    kcs[:, mine] = kv[0, own : own + tok, 0:hd]
    vcs[:, mine] = kv[0, own : own + tok, hd : 2 * hd]

    k_right[1].wait_recv()
    k_right[2] = go(
        remote(kv_at(0, base(-1) + first, half), kv_at(0, 0, half), ks.at[2], kr.at[2], seq(1))
    )
    to_other(base(-1), block)
    k_left[1].wait_recv()
    k_left[2] = go(
        remote(kv_at(0, base(1), first), kv_at(0, base(2), first), ks.at[3], kr.at[3], seq(-1))
    )
    to_other(base(1), block)

    step = [1]

    def w_step():
        nonlocal flight
        arrived = flight
        step[0] += 1
        if step[0] > nz // 2 + 1:
            return
        for copy, offset, part in arrived:
            copy.wait_recv()
        if step[0] <= nz // 2:
            flight = w_send(step[0])
        else:
            flight = []
        for copy, offset, part in arrived:
            w_other(offset, part)

    w_step()
    k_right[2].wait_recv()
    to_other(0, half)
    k_left[2].wait_recv()
    to_other(base(2), first)
    lane = iota((1, CORES * window), 1)
    kpos = jnp.full((1, CORES * window), -1, jnp.int32)
    for cc in range(CORES):
        core = c if cc == 0 else 1 - c
        for offset in range(1 - reach, reach + 1):
            rel = lane - (cc * window + base(offset))
            spot = order_ref[at_z(offset, core)] * tok + rel
            kpos = jnp.where((rel >= 0) & (rel < tok), spot, kpos)
    row = iota((rows, 1), 0)
    eye = iota((rows, hd), 0) == iota((rows, hd), 1)

    def partial(slot):
        for h in range(q_per):
            qrows[h * tok : (h + 1) * tok, :] = qbuf[slot, :, h * hd : (h + 1) * hd]
        qpos = order_ref[at_z(stride * slot)] * tok + lax.rem(row, tok)
        keys = kv[:, :, 0:hd].reshape(CORES * window, hd)
        values = kv[:, :, hd : 2 * hd].reshape(CORES * window, hd)
        s = lax.dot_general(
            qrows[...], keys, (((1,), (1,)), ((), ())), preferred_element_type=F32
        )
        s = jnp.where(kpos <= qpos, s * scale, -1e30)
        top = jnp.max(s, axis=1, keepdims=True)
        p = jnp.exp(s - top)
        total = jnp.sum(p, axis=1, keepdims=True)
        o = jnp.dot(p.astype(BF16), values, preferred_element_type=F32)
        return o / total, top + jnp.log(total)

    q_copies[1].wait_recv()
    q_copies[3].wait_recv()
    for copy in dies:
        copy.wait_recv()
    o_copies = {}
    for slot in (1, 3, 2):
        if slot == 2:
            q_copies[2].wait_recv()
        o, lse = partial(slot)
        osend[slot] = o.astype(BF16)
        lsend[slot] = jnp.broadcast_to(
            jnp.sum(jnp.where(eye, lse, 0.0), axis=0, keepdims=True), lsend.shape[1:]
        )
        to = (STRIDES - slot) % STRIDES
        o_copies[to] = (
            go(remote(osend.at[slot], orecv.at[to], os_.at[to], or_.at[to], seq(stride * slot))),
            go(remote(lsend.at[slot], lrecv.at[to], ls.at[to], lr.at[to], seq(stride * slot))),
        )
        w_step()
    o, lse = partial(0)
    w_step()
    outs, logs = [o], [lse]
    for slot in (1, 3, 2):
        for copy in o_copies[slot]:
            copy.wait_recv()
        outs.append(orecv[slot].astype(F32))
        logs.append(jnp.sum(jnp.where(eye, lrecv[slot][0:1, :], 0.0), axis=1, keepdims=True))
    top = functools.reduce(jnp.maximum, logs)
    shares = [jnp.exp(x - top) for x in logs]
    total = functools.reduce(jnp.add, shares)
    heads = functools.reduce(jnp.add, [a * b for a, b in zip(outs, shares)]) / total
    heads = heads.astype(BF16)
    for h in range(q_per):
        oall[r, :, h * hd : (h + 1) * hd] = heads[h * tok : (h + 1) * tok, :]
    x_copies = [
        go(remote(oall.at[r], oall.at[r], xs.at[j], xr.at[j], across[j])) for j in range(1, nr)
    ]
    while step[0] <= nz // 2:
        w_step()
    for copy in x_copies:
        copy.wait_recv()
    for copy in w_dies:
        copy.wait_recv()
    projected = jnp.zeros((tok, width), F32)
    for j in range(nr):
        projected = projected + jnp.dot(
            oall[j], wall[j * width : (j + 1) * width, :], preferred_element_type=F32
        )
    attended = (res_ref[...].astype(F32) + projected).astype(BF16)
    aall[r] = attended
    a_copies = [
        go(remote(aall.at[r], aall.at[r], as_.at[j], ar.at[j], across[j])) for j in range(1, nr)
    ]
    att_ref[...] = attended
    for copy in k_copies + v_copies:
        copy.wait_recv()
    kc_ref[...] = kcs[...]
    vc_ref[...] = vcs[...]
    for copy in a_copies:
        copy.wait_recv()
    full_ref[...] = aall[...]
    for copy in pending:
        copy.wait_send()


def experts_kernel(
    nz,
    nr,
    idv_ref,
    ids_ref,
    x_ref,
    gain_ref,
    router_ref,
    wg_ref,
    wu_ref,
    wd_ref,
    out_ref,
    wgu,
    wd,
    ring,
    rows_all,
    stacked,
    parts,
    right_in,
    left_in,
    mine,
    back,
    loc,
    ds,
    dr,
    gs,
    gr,
    rs,
    rr,
    xs,
    xr,
):
    z, c, r = place()
    _, tok, width = x_ref.shape
    hidden = wg_ref.shape[2]
    packed = nr * CAP
    padded = nr * tok
    n_parts = 2
    piece = packed // n_parts
    expert = lax.rem(r, EXPERTS)

    def seq(offset):
        return {"seq": lax.rem(z + (offset % nz), nz) * CORES + c}

    other = {"seq": z * CORES + (1 - c)}
    across = [{"rep": lax.rem(r + j, nr)} for j in range(nr)]
    up_at = CORES * hidden
    loads = [
        pltpu.make_async_copy(wg_ref.at[0], wgu.at[:, pl.ds(0, hidden)], loc.at[0]),
        pltpu.make_async_copy(wu_ref.at[0], wgu.at[:, pl.ds(up_at, hidden)], loc.at[1]),
        pltpu.make_async_copy(wd_ref.at[0], wd.at[pl.ds(0, hidden), :], loc.at[2]),
    ]
    for copy in loads:
        copy.start()
    greet([seq(1), seq(-1), other] + across[1:])
    pending = []

    def go(copy):
        copy.start()
        pending.append(copy)
        return copy

    x = x_ref[...].astype(F32)
    square = jnp.sum(jnp.sum(x * x, axis=0), axis=1, keepdims=True) / (nr * width)
    normed = (x * gain_ref[...].reshape(nr, 1, width) * lax.rsqrt(square + 1e-05)[None]).astype(BF16)

    lane = iota((1, padded), 1)
    line = iota((padded, 1), 0)
    lane_rank = jnp.full((1, padded), -padded, jnp.int32)
    line_rank = jnp.full((padded, 1), -padded, jnp.int32)
    count = jnp.int32(0)
    for t in range(tok):
        member = (ids_ref[t, 0] == expert) | (ids_ref[t, 1] == expert)
        rank = jnp.where(member, count, -padded)
        count = count + jnp.where(member, 1, 0)
        lane_rank = jnp.where(lax.rem(lane, tok) == t, rank, lane_rank)
        line_rank = jnp.where(lax.rem(line, tok) == t, rank, line_rank)

    def one_hot(mask):
        return jnp.where(mask, 1.0, 0.0).astype(BF16)

    choose = one_hot(iota((packed, padded), 0) == (lane // tok) * CAP + lane_rank)
    put_back = one_hot(iota((padded, packed), 1) == (line // tok) * CAP + line_rank)
    spot = lax.rem(line, tok)
    widen = one_hot(
        iota((padded, packed), 1) == jnp.where(spot < CAP, (line // tok) * CAP + spot, -1)
    )
    spot = lax.rem(lane, tok)
    narrow = one_hot(
        iota((packed, padded), 0) == jnp.where(spot < CAP, (lane // tok) * CAP + spot, -1)
    )

    ring[0] = jnp.dot(
        choose, normed.reshape(padded, width), preferred_element_type=F32
    ).astype(BF16)

    def part(ref, slot, p):
        return ref.at[slot, pl.ds(p * piece, piece), :]

    mid = nz // 2
    right, left = {}, {}

    def gather_send(t):
        for p in range(n_parts):
            if t < mid or p == 0:
                right[t, p] = go(
                    remote(part(ring, t - 1, p), part(ring, t, p), gs.at[0, t, p], gr.at[0, t, p], seq(1))
                )
            if t < mid or p == 1:
                left[t, p] = go(
                    remote(
                        part(ring, (nz - t + 1) % nz, p),
                        part(ring, nz - t, p),
                        gs.at[1, t, p],
                        gr.at[1, t, p],
                        seq(-1),
                    )
                )

    gather_send(1)
    swaps = [
        go(remote(wg_ref.at[0], wgu.at[:, pl.ds(hidden, hidden)], ds.at[0], dr.at[0], other)),
        go(remote(wu_ref.at[0], wgu.at[:, pl.ds(up_at + hidden, hidden)], ds.at[1], dr.at[1], other)),
        go(remote(wd_ref.at[0], wd.at[pl.ds(hidden, hidden), :], ds.at[2], dr.at[2], other)),
    ]

    logits = []
    for e in range(EXPERTS):
        column = router_ref[e * nr : (e + 1) * nr, :].reshape(nr, 1, width)
        logits.append(jnp.sum(jnp.sum(normed.astype(F32) * column, axis=0), axis=1, keepdims=True))
    one, two = idv_ref[:, 0:1], idv_ref[:, 1:2]
    first = functools.reduce(jnp.add, [jnp.where(one == e, logits[e], 0.0) for e in range(EXPERTS)])
    second = functools.reduce(jnp.add, [jnp.where(two == e, logits[e], 0.0) for e in range(EXPERTS)])
    share = jax.nn.sigmoid(first - second)
    shares = [
        jnp.where(one == e, share, 0.0) + jnp.where(two == e, 1.0 - share, 0.0)
        for e in range(EXPERTS)
    ]

    arrival = [0]
    for t in range(1, mid):
        arrival += [t, nz - t]
    arrival.append(mid)
    group = nz // 2

    def lay_out(i):
        wide = jnp.dot(widen, ring[arrival[i]], preferred_element_type=F32).astype(BF16)
        for f in range(nr):
            rows_all[i * tok : (i + 1) * tok, f * width : (f + 1) * width] = wide[
                f * tok : (f + 1) * tok, :
            ]

    def compute(start, count):
        sel = slice(start * tok, (start + count) * tok)
        gate = jnp.dot(rows_all[sel, :], wgu[:, 0:up_at], preferred_element_type=F32)
        up = jnp.dot(rows_all[sel, :], wgu[:, up_at : 2 * up_at], preferred_element_type=F32)
        act = (gate * jax.nn.sigmoid(gate) * up).astype(BF16)
        for f in range(nr):
            y = jnp.dot(
                act, wd[:, f * width : (f + 1) * width], preferred_element_type=F32
            ).astype(BF16)
            for i in range(count):
                stacked[start + i, f * tok : (f + 1) * tok, :] = y[i * tok : (i + 1) * tok, :]
        for i in range(start, start + count):
            parts[arrival[i]] = jnp.dot(
                narrow, stacked[i], preferred_element_type=F32
            ).astype(BF16)

    lay_out(0)
    for t in range(1, mid + 1):
        for p in range(n_parts):
            if (t, p) in right:
                right[t, p].wait_recv()
            if (t, p) in left:
                left[t, p].wait_recv()
        if t < mid:
            gather_send(t + 1)
            lay_out(2 * t - 1)
            lay_out(2 * t)
        if t == mid // 2:
            for copy in loads:
                copy.wait()
            for copy in swaps:
                copy.wait_recv()
            compute(0, group)
    lay_out(nz - 1)
    compute(group, nz - group)

    sums = {}

    def reduce_send(way, t, p, src):
        into = right_in if way == 0 else left_in
        sums[way, t, p] = go(
            remote(src, part(into, t, p), rs.at[way, t, p], rr.at[way, t, p], seq(1 if way == 0 else -1))
        )

    def behind(way, t):
        return (nz - t) % nz if way == 0 else t % nz

    def begins(way, p):
        return mid if p == way else mid - 1

    for t in range(mid, 0, -1):
        for p in range(n_parts):
            for way in (0, 1):
                if t > begins(way, p):
                    continue
                slot = behind(way, t)
                if t == begins(way, p):
                    reduce_send(way, t, p, part(parts, slot, p))
                    continue
                into = right_in if way == 0 else left_in
                sums[way, t + 1, p].wait_recv()
                sel = slice(p * piece, (p + 1) * piece)
                into[t + 1, sel, :] = (
                    into[t + 1, sel, :].astype(F32) + parts[slot, sel, :].astype(F32)
                ).astype(BF16)
                reduce_send(way, t, p, part(into, t + 1, p))
    for p in range(n_parts):
        for way in (0, 1):
            sums[way, 1, p].wait_recv()
    total = (
        parts[0].astype(F32) + right_in[1].astype(F32) + left_in[1].astype(F32)
    ).astype(BF16)
    mine[...] = (
        jnp.dot(put_back, total, preferred_element_type=F32).astype(BF16).reshape(nr, tok, width)
    )
    x_copies = [
        go(remote(mine.at[lax.rem(r + j, nr)], back.at[r], xs.at[j], xr.at[j], across[j]))
        for j in range(1, nr)
    ]
    back[r] = mine[r]
    for copy in x_copies:
        copy.wait_recv()
    out = x_ref[r].astype(F32)
    for j in range(nr):
        out = out + shares[j % EXPERTS] * back[j].astype(F32)
    out_ref[...] = out.astype(BF16)
    for copy in pending:
        copy.wait_send()


def body(
    nz,
    nr,
    queries,
    keys_new,
    values_new,
    keys_past,
    values_past,
    block_order,
    residual,
    out_proj,
    norm_gain,
    router,
    w_gate,
    w_up,
    w_down,
    expert_ids,
):
    tok, width = queries.shape
    hd = keys_new.shape[1]
    past = keys_past.shape[0]
    q_per = width // hd
    rows = tok * q_per
    depth = out_proj.shape[0]
    hidden = w_gate.shape[2]
    model = nr * width
    window = (nz // STRIDES) * (past + tok)
    dma = pltpu.SemaphoreType.DMA
    vmem = pl.BlockSpec(memory_space=pltpu.VMEM)
    smem = pl.BlockSpec(memory_space=pltpu.SMEM)
    hbm = pl.BlockSpec(memory_space=pl.ANY)

    attended, full, keys_cache, values_cache = pl.pallas_call(
        functools.partial(attention_kernel, nz, nr),
        out_shape=(
            jax.ShapeDtypeStruct((tok, width), BF16),
            jax.ShapeDtypeStruct((nr, tok, width), BF16),
            jax.ShapeDtypeStruct((tok, nr * hd), BF16),
            jax.ShapeDtypeStruct((tok, nr * hd), BF16),
        ),
        in_specs=[smem, hbm, hbm, hbm, hbm, hbm, vmem, hbm],
        out_specs=(vmem, vmem, vmem, vmem),
        scratch_shapes=[
            pltpu.VMEM((STRIDES, tok, width), BF16),
            pltpu.VMEM((rows, hd), BF16),
            pltpu.VMEM((CORES, window, 2 * hd), BF16),
            pltpu.VMEM((CORES * nz * depth, width), BF16),
            pltpu.VMEM((STRIDES, rows, hd), BF16),
            pltpu.VMEM((STRIDES, 8, hd), F32),
            pltpu.VMEM((STRIDES, rows, hd), BF16),
            pltpu.VMEM((STRIDES, 8, hd), F32),
            pltpu.VMEM((nr, tok, width), BF16),
            pltpu.VMEM((nr, tok, width), BF16),
            pltpu.VMEM((tok, nr * hd), BF16),
            pltpu.VMEM((tok, nr * hd), BF16),
            dma((6,)),
            dma((STRIDES,)),
            dma((STRIDES,)),
            dma((4,)),
            dma((4,)),
            dma((5,)),
            dma((5,)),
            dma((nz,)),
            dma((nz,)),
            dma((nz + 1,)),
            dma((nz + 1,)),
            dma((nr,)),
            dma((nr,)),
            dma((nr,)),
            dma((nr,)),
            dma((STRIDES,)),
            dma((STRIDES,)),
            dma((STRIDES,)),
            dma((STRIDES,)),
            dma((nr,)),
            dma((nr,)),
            dma((nr,)),
            dma((nr,)),
        ],
        compiler_params=pltpu.CompilerParams(collective_id=0, has_side_effects=True),
        name="attention",
    )(
        block_order,
        queries,
        keys_new,
        values_new,
        keys_past,
        values_past,
        residual,
        out_proj,
    )
    packed = nr * CAP
    padded = nr * tok
    layer_out = pl.pallas_call(
        functools.partial(experts_kernel, nz, nr),
        out_shape=jax.ShapeDtypeStruct((tok, width), BF16),
        in_specs=[vmem, smem, vmem, vmem, vmem, hbm, hbm, hbm],
        out_specs=vmem,
        scratch_shapes=[
            pltpu.VMEM((model, 2 * CORES * hidden), BF16),
            pltpu.VMEM((CORES * hidden, model), BF16),
            pltpu.VMEM((nz, packed, width), BF16),
            pltpu.VMEM((nz * tok, model), BF16),
            pltpu.VMEM((nz, padded, width), BF16),
            pltpu.VMEM((nz, packed, width), BF16),
            pltpu.VMEM((nz // 2 + 1, packed, width), BF16),
            pltpu.VMEM((nz // 2 + 1, packed, width), BF16),
            pltpu.VMEM((nr, tok, width), BF16),
            pltpu.VMEM((nr, tok, width), BF16),
            dma((3,)),
            dma((3,)),
            dma((3,)),
            dma((2, nz // 2 + 1, 2)),
            dma((2, nz // 2 + 1, 2)),
            dma((2, nz // 2 + 1, 2)),
            dma((2, nz // 2 + 1, 2)),
            dma((nr,)),
            dma((nr,)),
        ],
        compiler_params=pltpu.CompilerParams(collective_id=1, has_side_effects=True),
        name="experts",
    )(
        expert_ids,
        expert_ids,
        full,
        norm_gain.reshape(nr, width),
        router.T.reshape(EXPERTS * nr, width),
        w_gate,
        w_up,
        w_down,
    )
    return attended, layer_out, keys_cache, values_cache


def solution(mesh):
    nz = mesh.shape["seq"] // CORES
    nr = mesh.shape["rep"]
    rows = P(("groups", "seq"), "rep")
    whole = P(("groups", "seq"), None)
    return jax.shard_map(
        functools.partial(body, nz, nr),
        mesh=mesh,
        in_specs=(
            rows,
            rows,
            rows,
            rows,
            rows,
            P("groups"),
            rows,
            P("seq", "rep"),
            P(),
            P(),
            P("rep", None, "seq"),
            P("rep", None, "seq"),
            P("rep", "seq", None),
            whole,
        ),
        out_specs=(rows, rows, whole, whole),
        check_vma=False,
    )
```
